32 devices in a mesh: task: 4 (over y, x), tok: 8 (over z, core).
Axes of the slice: x: 2, y: 2, z: 4, core: 2. Of those that a mesh axis runs over, the one named last changes fastest.
Arguments:
- hidden: bfloat16 [4, 256, 3584], P('task', 'tok'), may hold values from -6 to 6
- attn_out: bfloat16 [4, 256, 3584], P('task', 'tok'), may hold values from -6 to 6
- gain_attn: bfloat16 [3584], replicated, may hold values from 0.5 to 1.5
- gain_mlp: bfloat16 [3584], replicated, may hold values from 0.5 to 1.5
- lengths: int32 [4, 2], P('task'), may hold values from 32 to 128
Outputs:
- gram_attn: float32 [8, 896, 1792], P('tok', 'task')
- gram_mlp: float32 [8, 896, 1792], P('tok', 'task')
The draws below stay inside these ranges and needn't reach their ends.
All inputs are finite; a program needn't handle non-finite values.
Results may differ from the reference program's by a relative error of at most 0.0044.
Values may be sent and summed in bfloat16 or wider, within the bound.
A program may use at most 64 MiB of HBM per device.

```python
import jax
import jax.numpy as jnp
from jax import lax

D = 3584
SEQS = 2
BSIDE = 2
BW = 1792
PR = 896
TOKENS = 256
SEQ_LEN = 128
N_TASK = 4
N_TOK = 8


def with_ends(result, stream_key, smallest, largest):
    longest = result.shape.index(max(result.shape))
    spots = []
    for shift in (0, 1):
        where = [jax.random.randint(jax.random.fold_in(stream_key, axis), (), 0, length) for axis, length in enumerate(result.shape)]
        where[longest] = (where[longest] + shift) % result.shape[longest]
        spots.append(tuple(where))
    return result.at[spots[0]].set(smallest).at[spots[1]].set(largest)


def block_levels(stream_key, shape, shards, least, high):
    loudness = 1.0
    for position, blocks in shards:
        steps = jax.random.uniform(jax.random.fold_in(jax.random.fold_in(stream_key, 6), position), (blocks,), jnp.float32, least / len(shards), high / len(shards))
        loudness = loudness * jnp.repeat(jnp.exp(steps), shape[position] // blocks).reshape((-1,) + (1,) * (len(shape) - 1 - position))
    return loudness


def scatter_about(rng, dims, scale, most, split=(), kind=jnp.bfloat16):
    drawn = scale * jax.random.normal(rng, dims, jnp.float32)
    if split:
        drawn = drawn * block_levels(rng, dims, split, -0.22, 0.18)
    return jnp.clip(drawn, -most, most).astype(kind)


def setup_inputs(seed: int = 0) -> dict:
    key_list = jax.random.split(jax.random.key(seed), 6)
    return {
        "hidden": scatter_about(key_list[0], (N_TASK, TOKENS, D), 1.0, 6.0, ((0, 4), (1, 8))),
        "attn_out": scatter_about(key_list[1], (N_TASK, TOKENS, D), 1.0, 6.0, ((0, 4), (1, 8))),
        "gain_attn": jnp.clip(1.0 + 0.1 * jax.random.normal(key_list[2], (D,), jnp.float32), 0.5, 1.5).astype(jnp.bfloat16),
        "gain_mlp": jnp.clip(1.0 + 0.1 * jax.random.normal(key_list[3], (D,), jnp.float32), 0.5, 1.5).astype(jnp.bfloat16),
        "lengths": with_ends(jax.random.randint(key_list[4], (N_TASK, SEQS), SEQ_LEN // 4, SEQ_LEN + 1), jax.random.fold_in(key_list[4], 1), SEQ_LEN // 4, SEQ_LEN).astype(jnp.int32),
    }


def normed(values, gain):
    scale = lax.rsqrt(lax.optimization_barrier(jnp.mean(values * values, axis=-1, keepdims=True)) + 1e-06)
    return values * scale * gain.astype(jnp.float32)

def reference(hidden, attn_out, gain_attn, gain_mlp, lengths):
    place = jnp.arange(TOKENS, dtype=jnp.int32)
    which = place // SEQ_LEN
    offset = place % SEQ_LEN
    total_attn = jnp.zeros((D, D), jnp.float32)
    total_mlp = jnp.zeros((D, D), jnp.float32)
    for group in range(N_TASK):
        limit = lengths[group][which]
        live = (offset < limit).astype(jnp.float32)[:, None]
        first = hidden[group].astype(jnp.float32)
        x_attn = (normed(first, gain_attn) * live).astype(jnp.bfloat16)
        mixed = first + attn_out[group].astype(jnp.float32)
        x_mlp = (normed(mixed, gain_mlp) * live).astype(jnp.bfloat16)
        total_attn = total_attn + jnp.dot(x_attn.T, x_attn, preferred_element_type=jnp.float32)
        total_mlp = total_mlp + jnp.dot(x_mlp.T, x_mlp, preferred_element_type=jnp.float32)

    def tiled(total):
        gram = total / TOKENS
        blocks = gram.reshape(BSIDE, BW, BSIDE, BW).transpose(0, 2, 1, 3)
        return blocks.reshape(N_TOK, PR, BW)
    return (tiled(total_attn), tiled(total_mlp))
```

```python
import functools

import jax
import jax.numpy as jnp
from jax import lax
from jax.experimental import pallas as pl
from jax.experimental.pallas import tpu as pltpu
from jax.sharding import PartitionSpec as P

LANES = 128


def gather_kernel(
    hidden, attn_out, gain_attn, gain_mlp, lengths, out_attn, out_mlp,
    mine, held, rows, total, got, row_got, row_sent, z_sent, side_sent, pair_sent,
):
    task, tok = lax.axis_index("task"), lax.axis_index("tok")
    n_task = lax.axis_size("task")
    plane, core = tok // 2, tok % 2
    band = plane % 2
    tok_dev, column_band = held.shape[2], held.shape[3]
    n_planes = held.shape[1] // (2 * n_task)
    inner = jnp.logical_or(plane == 1, plane == 2)
    outer = jnp.logical_not(inner)

    def flip(value, bit):
        return value + bit - 2 * bit * (value // bit % 2)

    task_x, task_y = flip(task, 1), flip(task, 2)
    task_d = flip(task_x, 2)
    plane_1, plane_2 = flip(plane, 1), flip(plane, 2)
    plane_3 = flip(plane_1, 2)
    near, far = jnp.where(inner, plane_3, plane_2), jnp.where(inner, plane_2, plane_3)
    order = (plane, plane_1, near, far)

    def at(tasks, planes, cores):
        return {"task": tasks, "tok": planes * 2 + cores}

    def chunk(planes, tasks, cores):
        return planes * (2 * n_task) + tasks * 2 + cores

    own = chunk(plane, task, core)

    slab = 16
    seq_count = lengths.shape[1]
    seq_slots = tok_dev * lax.axis_size("tok") // seq_count
    for low in range(0, tok_dev, slab):
        part = pl.ds(low, slab)
        place = tok * tok_dev + low + lax.broadcasted_iota(jnp.int32, (slab, 1), 0)
        live = jnp.zeros((slab, 1), jnp.float32)
        for seq in range(seq_count):
            offset = place - seq * seq_slots
            inside = (offset >= 0) & (offset < seq_slots) & (offset < lengths[0, seq])
            live = jnp.where(inside, 1.0, live)
        first = hidden[0, part, :].astype(jnp.float32)
        mixed = first + attn_out[0, part, :].astype(jnp.float32)
        for which, values, gain in ((0, first, gain_attn), (1, mixed, gain_mlp)):
            done = (normed(values, gain[...]) * live).astype(jnp.bfloat16)
            for side in range(2):
                mine[which, side, part, :] = done[:, side * column_band : (side + 1) * column_band]
    for which in range(2):
        held[which, own] = mine[which, band]

    peers = (
        at(task_x, plane, core), at(task_y, plane, core), at(task, plane, 1 - core),
        at(task, plane_1, core), at(task, plane_2, core), at(task, plane_3, core),
    )
    barrier = pltpu.get_barrier_semaphore()
    for peer in peers:
        pl.semaphore_signal(
            barrier, inc=1, device_id=peer, device_id_type=pl.DeviceIdType.MESH
        )
    pl.semaphore_wait(barrier, len(peers))
    to_x, to_y, to_pair, to_1, to_2, to_3 = peers

    def copy(source, which, q, sent, peer):
        return pltpu.make_async_remote_copy(
            src_ref=source, dst_ref=held.at[which, q], send_sem=sent,
            recv_sem=got.at[which, q], device_id=peer,
            device_id_type=pl.DeviceIdType.MESH,
        )

    started = []

    def send(*arguments):
        out = copy(*arguments)
        out.start()
        started.append(out)

    def arrive(which, q):
        copy(held.at[which, q], which, q, pair_sent.at[which, q], to_pair).wait_recv()

    def to_inner(which):
        return copy(mine.at[which, 1 - band], which, own, z_sent.at[which, 2], to_3)

    def relay(which):
        q = chunk(plane_1, task, core)
        return copy(held.at[which, q], which, q, z_sent.at[which, 3], to_2)

    def own_step(step):
        for which in range(2):
            q = chunk(order[step], task, core)
            if step:
                arrive(which, q)
                source = held.at[which, q]
            else:
                source = mine.at[which, band]
            if step == 1:
                @pl.when(inner)
                def _():
                    relay(which).start()
            send(source, which, q, side_sent.at[0, which, step], to_x)
            send(source, which, q, side_sent.at[1, which, step], to_y)
            if step == 0:
                @pl.when(inner)
                def _():
                    to_inner(which).start()
                send(mine.at[which, 1 - band], which, own, z_sent.at[which, 0], to_1)
                send(source, which, own, z_sent.at[which, 1], to_2)
            send(source, which, q, pair_sent.at[which, q], to_pair)

    def side_step(step):
        for which in range(2):
            for tasks, relayed, axis, peer in (
                (task_x, 0, 1, to_y), (task_y, 1, 0, to_x)
            ):
                q = chunk(order[step], tasks, core)
                arrive(which, q)
                if which == relayed:
                    send(
                        held.at[which, q], which, q,
                        side_sent.at[axis, which, n_planes + step], peer,
                    )
                send(held.at[which, q], which, q, pair_sent.at[which, q], to_pair)

    def diagonal_step(step):
        for which in range(2):
            q = chunk(order[step], task_d, core)
            arrive(which, q)
            send(held.at[which, q], which, q, pair_sent.at[which, q], to_pair)

    row_count = out_attn.shape[1]
    padded = rows.shape[3]
    window = min(padded + LANES, column_band)
    row_start = core * (column_band // 2) + task * row_count
    base = jnp.minimum(row_start // LANES * LANES, column_band - window)
    shift = window - (row_start - base)

    def row_copy(group):
        return pltpu.make_async_remote_copy(
            src_ref=rows.at[group], dst_ref=rows.at[group], send_sem=row_sent.at[group],
            recv_sem=row_got.at[group], device_id=to_1,
            device_id_type=pl.DeviceIdType.MESH,
        )

    def rows_of(step, tasks, other_arrived=True):
        for which in range(2):
            arrive(which, chunk(order[step], tasks, 1 - core))
        group = order[step] * n_task + tasks

        @pl.when(outer)
        def _():
            for which in range(2):
                span = held[
                    which, pl.ds(group * 2, 2), :, pl.ds(pl.multiple_of(base, LANES), window)
                ]
                span = span.reshape(2 * tok_dev, window).astype(jnp.float32)
                span = pltpu.roll(span, shift, 1)
                rows[group, which] = span[:, :padded].astype(jnp.bfloat16)

        return group

    def send_rows(group):
        @pl.when(outer)
        def _():
            row_copy(group).start()

    def cut(step, members):
        waiting = None
        for tasks in members:
            group = rows_of(step, tasks)
            if waiting is not None:
                send_rows(waiting)
            waiting = group
        return waiting

    def product(step, which):
        left = rows[pl.ds(order[step] * n_task, n_task), which]
        right = held[which, pl.ds(order[step] * 2 * n_task, 2 * n_task)]
        depth = 2 * n_task * tok_dev
        return lax.dot_general(
            left.reshape(depth, padded), right.reshape(depth, column_band),
            (((0,), (0,)), ((), ())), preferred_element_type=jnp.float32,
        )

    def rows_arrive(step):
        @pl.when(inner)
        def _():
            for tasks in range(n_task):
                row_copy(order[step] * n_task + tasks).wait_recv()

    def multiply(step):
        rows_arrive(step)

        @pl.loop(0, 2)
        def _(which):
            piece = product(step, which)
            if step == 0:
                total[which] = piece
            else:
                total[which] += piece

    sides = (task, task_x, task_y)
    own_step(0)
    own_step(1)
    side_step(0)
    own_step(2)
    side_step(1)
    diagonal_step(0)
    waiting = cut(0, sides + (task_d,))
    own_step(3)
    send_rows(waiting)
    side_step(2)
    diagonal_step(1)
    waiting = cut(1, sides + (task_d,))
    multiply(0)
    send_rows(waiting)
    waiting = cut(2, sides)
    side_step(3)
    send_rows(waiting)
    diagonal_step(2)
    waiting = cut(2, (task_d,))
    multiply(1)
    send_rows(waiting)
    waiting = cut(3, sides)
    diagonal_step(3)
    send_rows(waiting)
    waiting = cut(3, (task_d,))
    multiply(2)
    send_rows(waiting)
    rows_arrive(3)
    factor = 1.0 / (tok_dev * lax.axis_size("tok"))
    for which, out in ((0, out_attn), (1, out_mlp)):
        piece = total[which] + product(3, which)
        out[0] = piece[:row_count] * factor

    for out in started:
        out.wait_send()

    @pl.when(inner)
    def _():
        for which in range(2):
            to_inner(which).wait_send()
            relay(which).wait_send()

    @pl.when(outer)
    def _():
        for group in range(n_planes * n_task):
            row_copy(group).wait_send()


def gathered(hidden, attn_out, gain_attn, gain_mlp, lengths):
    _, tok_dev, width = hidden.shape
    n_tok, n_task = lax.axis_size("tok"), lax.axis_size("task")
    column_band = width // 2
    row_count = column_band // 2 // n_task
    padded = -(-row_count // LANES) * LANES
    devices = n_tok * n_task
    groups = devices // 2
    vmem = pl.BlockSpec(memory_space=pltpu.VMEM)
    shape = jax.ShapeDtypeStruct((1, row_count, column_band), jnp.float32)
    semaphores = pltpu.SemaphoreType.DMA
    return pl.pallas_call(
        gather_kernel,
        out_shape=(shape, shape),
        in_specs=[vmem] * 4 + [pl.BlockSpec(memory_space=pltpu.SMEM)],
        out_specs=(vmem, vmem),
        scratch_shapes=[
            pltpu.VMEM((2, 2, tok_dev, column_band), jnp.bfloat16),
            pltpu.VMEM((2, devices, tok_dev, column_band), jnp.bfloat16),
            pltpu.VMEM((groups, 2, 2 * tok_dev, padded), jnp.bfloat16),
            pltpu.VMEM((2, padded, column_band), jnp.float32),
            semaphores((2, devices)),
            semaphores((groups,)),
            semaphores((groups,)),
            semaphores((2, 4)),
            semaphores((2, 2, n_tok)),
            semaphores((2, devices)),
        ],
        compiler_params=pltpu.CompilerParams(
            collective_id=0, has_side_effects=True, vmem_limit_bytes=48 * 2**20
        ),
    )(hidden, attn_out, gain_attn.reshape(1, width), gain_mlp.reshape(1, width), lengths)


def from_partner(block, axis, distance):
    count = lax.axis_size(axis)
    route = []
    for low in range(count):
        high = low | 1 << distance
        if high != low and high < count:
            route += [(low, high), (high, low)]
    return lax.ppermute(block, axis, route)


def normed(values, gain):
    scale = lax.rsqrt(jnp.mean(values * values, axis=-1, keepdims=True) + 1e-06)
    return values * scale * gain.astype(jnp.float32)


def per_device(hidden, attn_out, gain_attn, gain_mlp, lengths):
    tok_dev = hidden.shape[1]
    width = hidden.shape[2]
    n_tok = lax.axis_size("tok")
    n_task = lax.axis_size("task")
    block_side = min(4, max(2, n_tok // 16))
    token_parts = n_tok // (block_side * block_side)
    if (n_task, n_tok, block_side) == (4, 8, 2) and width % (4 * LANES) == 0 and tok_dev % 16 == 0:
        return gathered(hidden, attn_out, gain_attn, gain_mlp, lengths)
    column_band = width // block_side
    tile_rows = column_band // token_parts
    slice_rows = tok_dev // token_parts
    seq_count = lengths.shape[1]
    seq_slots = tok_dev * n_tok // seq_count
    place = lax.axis_index("tok") * tok_dev + jnp.arange(tok_dev, dtype=jnp.int32)
    which = place // seq_slots
    offset = place % seq_slots
    owner = which[:, None] == jnp.arange(seq_count, dtype=jnp.int32)[None, :]
    limit = jnp.sum(jnp.where(owner, lengths[0][None, :], 0), axis=1)
    live = (offset < limit).astype(jnp.float32)[:, None]
    first = hidden[0].astype(jnp.float32)
    x_attn = (normed(first, gain_attn) * live).astype(jnp.bfloat16)
    mixed = first + attn_out[0].astype(jnp.float32)
    x_mlp = (normed(mixed, gain_mlp) * live).astype(jnp.bfloat16)

    def bands(values):
        split = values.reshape(token_parts, slice_rows, block_side, column_band).transpose(
            2, 0, 1, 3
        )
        shape = (block_side, block_side, token_parts, slice_rows, column_band)
        left_side = jnp.broadcast_to(split[:, None], shape).reshape(n_tok, slice_rows, column_band)
        right_side = jnp.broadcast_to(split[None], shape).reshape(n_tok, slice_rows, column_band)
        return (left_side, right_side)

    left_attn, right_attn = bands(x_attn)
    left_mlp, right_mlp = bands(x_mlp)
    arrived = (
        lax.all_to_all(left_attn, "tok", split_axis=0, concat_axis=0, tiled=True),
        lax.all_to_all(right_attn, "tok", split_axis=0, concat_axis=0, tiled=True),
        lax.all_to_all(left_mlp, "tok", split_axis=0, concat_axis=0, tiled=True),
        lax.all_to_all(right_mlp, "tok", split_axis=0, concat_axis=0, tiled=True),
    )
    contract = (((0, 1), (0, 1)), ((), ()))
    tile_attn = lax.dot_general(
        arrived[0], arrived[1], contract, preferred_element_type=jnp.float32
    )
    tile_mlp = lax.dot_general(arrived[2], arrived[3], contract, preferred_element_type=jnp.float32)
    grams = (
        tile_attn.reshape(token_parts, tile_rows, column_band),
        tile_mlp.reshape(token_parts, tile_rows, column_band),
    )
    part_index = lax.axis_index("tok") % token_parts
    depth_bits = token_parts.bit_length() - 1

    def halve(current, bit):
        upper_bit = part_index // (1 << bit) % 2 == 1
        middle = current[0].shape[0] // 2
        outgoing = tuple(
            (jnp.where(upper_bit, piece[:middle], piece[middle:]) for piece in current)
        )
        kept = tuple((jnp.where(upper_bit, piece[middle:], piece[:middle]) for piece in current))
        incoming = from_partner(outgoing, "tok", bit)
        return tuple((mine + theirs for mine, theirs in zip(kept, incoming)))

    for bit in range(depth_bits - 1, -1, -1):
        grams = halve(grams, bit)
    shaped = tuple((piece.reshape(n_task, tile_rows // n_task, column_band) for piece in grams))
    grams = lax.psum_scatter(shaped, "task", scatter_dimension=0, tiled=True)
    factor = 1.0 / (tok_dev * n_tok)
    final_attn = grams[0] * factor
    final_mlp = grams[1] * factor
    return (final_attn, final_mlp)


def solution(mesh):
    return jax.shard_map(
        per_device,
        mesh=mesh,
        in_specs=(P("task", "tok", None), P("task", "tok", None), P(), P(), P("task", None)),
        out_specs=(P("tok", "task", None), P("tok", "task", None)),
        check_vma=False,
    )
```

```python
import functools

import jax
import jax.numpy as jnp
from jax import lax
from jax.experimental import pallas as pl
from jax.experimental.pallas import tpu as pltpu
from jax.sharding import PartitionSpec as P

LANES = 128


def planes_in_product_order():
    plane = lax.axis_index("tok") // 2
    inner = jnp.logical_or(plane == 1, plane == 2)
    plane_1 = plane + 1 - 2 * (plane % 2)
    plane_2 = jnp.where(plane // 2 == 1, plane - 2, plane + 2)
    plane_3 = 3 - plane
    return (
        jnp.where(inner, plane_1, plane), jnp.where(inner, plane, plane_1),
        jnp.where(inner, plane_3, plane_2), jnp.where(inner, plane_2, plane_3),
    )


def product(rows, held, plane, which, columns=slice(None)):
    n_task = lax.axis_size("task")
    left = rows[pl.ds(plane * n_task, n_task), which]
    right = held[which, pl.ds(plane * 2 * n_task, 2 * n_task), :, columns]
    depth = left.shape[0] * left.shape[1]
    return lax.dot_general(
        left.reshape(depth, left.shape[2]), right.reshape(depth, right.shape[2]),
        (((0,), (0,)), ((), ())), preferred_element_type=jnp.float32,
    )


def last_kernel(held, rows, total, out_attn, out_mlp, staged, sent):
    row_count, column_band = out_attn.shape[1], out_attn.shape[2]
    plane = planes_in_product_order()[3]
    factor = 1.0 / (lax.axis_size("tok") * held.shape[2])
    n_bands = sent.shape[1]
    width = column_band // n_bands
    writes = []
    for which, out in ((0, out_attn), (1, out_mlp)):
        for band in range(n_bands):
            span = slice(band * width, (band + 1) * width)
            piece = total[which, :, span] + product(rows, held, plane, which, span)
            staged[which, 0, :, span] = piece[:row_count] * factor
            write = pltpu.make_async_copy(
                staged.at[which, :, :, span], out.at[:, :, span], sent.at[which, band]
            )
            write.start()
            writes.append(write)
    for write in writes:
        write.wait()


def gather_kernel(
    hidden_hbm, attn_hbm, gain_attn_hbm, gain_mlp_hbm, lengths_hbm, held, rows, total,
    hidden, attn_out, gain_attn, gain_mlp, lengths, mine,
    loaded, got, row_got, row_sent, z_sent, side_sent, pair_sent,
):
    task, tok = lax.axis_index("task"), lax.axis_index("tok")
    n_task = lax.axis_size("task")
    plane, core = tok // 2, tok % 2
    band = plane % 2
    tok_dev, column_band = held.shape[2], held.shape[3]
    n_planes = held.shape[1] // (2 * n_task)
    inner = jnp.logical_or(plane == 1, plane == 2)
    outer = jnp.logical_not(inner)

    def flip(value, bit):
        return value + bit - 2 * bit * (value // bit % 2)

    task_x, task_y = flip(task, 1), flip(task, 2)
    task_d = flip(task_x, 2)
    plane_1, plane_2 = flip(plane, 1), flip(plane, 2)
    plane_3 = flip(plane_1, 2)
    near, far = jnp.where(inner, plane_3, plane_2), jnp.where(inner, plane_2, plane_3)
    order = (plane, plane_1, near, far)
    product_order = planes_in_product_order()

    def at(tasks, planes, cores):
        return {"task": tasks, "tok": planes * 2 + cores}

    def chunk(planes, tasks, cores):
        return planes * (2 * n_task) + tasks * 2 + cores

    own = chunk(plane, task, core)

    loads = [
        pltpu.make_async_copy(source, target, loaded.at[spot])
        for spot, (source, target) in enumerate((
            (hidden_hbm, hidden), (attn_hbm, attn_out), (gain_attn_hbm, gain_attn),
            (gain_mlp_hbm, gain_mlp), (lengths_hbm, lengths),
        ))
    ]
    for load in loads:
        load.start()
    peers = (
        at(task_x, plane, core), at(task_y, plane, core), at(task, plane, 1 - core),
        at(task, plane_1, core), at(task, plane_2, core), at(task, plane_3, core),
    )
    barrier = pltpu.get_barrier_semaphore()
    for peer in peers:
        pl.semaphore_signal(
            barrier, inc=1, device_id=peer, device_id_type=pl.DeviceIdType.MESH
        )
    for load in loads:
        load.wait()

    slab = 16
    seq_count = lengths.shape[1]
    seq_slots = tok_dev * lax.axis_size("tok") // seq_count
    for low in range(0, tok_dev, slab):
        part = pl.ds(low, slab)
        place = tok * tok_dev + low + lax.broadcasted_iota(jnp.int32, (slab, 1), 0)
        live = jnp.zeros((slab, 1), jnp.float32)
        for seq in range(seq_count):
            offset = place - seq * seq_slots
            inside = (offset >= 0) & (offset < seq_slots) & (offset < lengths[0, seq])
            live = jnp.where(inside, 1.0, live)
        first = hidden[0, part, :].astype(jnp.float32)
        mixed = first + attn_out[0, part, :].astype(jnp.float32)
        for which, values, gain in ((0, first, gain_attn), (1, mixed, gain_mlp)):
            done = (normed(values, gain[...].reshape(1, -1)) * live).astype(jnp.bfloat16)
            for side in range(2):
                mine[which, side, part, :] = done[:, side * column_band : (side + 1) * column_band]
    for which in range(2):
        held[which, own] = mine[which, band]

    pl.semaphore_wait(barrier, len(peers))
    to_x, to_y, to_pair, to_1, to_2, to_3 = peers

    def copy(source, which, q, sent, peer):
        return pltpu.make_async_remote_copy(
            src_ref=source, dst_ref=held.at[which, q], send_sem=sent,
            recv_sem=got.at[which, q], device_id=peer,
            device_id_type=pl.DeviceIdType.MESH,
        )

    started = []

    def send(*arguments):
        out = copy(*arguments)
        out.start()
        started.append(out)

    def arrive(which, q):
        copy(held.at[which, q], which, q, pair_sent.at[which, q], to_pair).wait_recv()

    def to_inner(which):
        return copy(mine.at[which, 1 - band], which, own, z_sent.at[which, 2], to_3)

    def relay(which):
        q = chunk(plane_1, task, core)
        return copy(held.at[which, q], which, q, z_sent.at[which, 3], to_2)

    def own_step(step, which):
        q = chunk(order[step], task, core)
        if step:
            arrive(which, q)
            source = held.at[which, q]
        else:
            source = mine.at[which, band]
        if step == 1:
            @pl.when(inner)
            def _():
                relay(which).start()
        send(source, which, q, side_sent.at[0, which, step], to_x)
        send(source, which, q, side_sent.at[1, which, step], to_y)
        if step == 0:
            @pl.when(inner)
            def _():
                to_inner(which).start()
            send(mine.at[which, 1 - band], which, own, z_sent.at[which, 0], to_1)
            send(source, which, own, z_sent.at[which, 1], to_2)
        send(source, which, q, pair_sent.at[which, q], to_pair)

    def side_step(step, which):
        for tasks, relayed, axis, peer in (
            (task_x, 0, 1, to_y), (task_y, 1, 0, to_x)
        ):
            q = chunk(order[step], tasks, core)
            arrive(which, q)
            if which == relayed:
                send(
                    held.at[which, q], which, q,
                    side_sent.at[axis, which, n_planes + step], peer,
                )
            send(held.at[which, q], which, q, pair_sent.at[which, q], to_pair)

    def diagonal_step(step, which):
        q = chunk(order[step], task_d, core)
        arrive(which, q)
        send(held.at[which, q], which, q, pair_sent.at[which, q], to_pair)

    row_count = column_band // 2 // n_task
    padded = rows.shape[3]
    window = min(padded + LANES, column_band)
    row_start = core * (column_band // 2) + task * row_count
    base = jnp.minimum(row_start // LANES * LANES, column_band - window)
    shift = window - (row_start - base)

    def row_copy(group):
        return pltpu.make_async_remote_copy(
            src_ref=rows.at[group], dst_ref=rows.at[group], send_sem=row_sent.at[group],
            recv_sem=row_got.at[group], device_id=to_1,
            device_id_type=pl.DeviceIdType.MESH,
        )

    def rows_of(step, tasks, other_arrived=True):
        for which in range(2):
            arrive(which, chunk(order[step], tasks, 1 - core))
        group = order[step] * n_task + tasks

        @pl.when(outer)
        def _():
            for which in range(2):
                span = held[
                    which, pl.ds(group * 2, 2), :, pl.ds(pl.multiple_of(base, LANES), window)
                ]
                span = span.reshape(2 * tok_dev, window).astype(jnp.float32)
                span = pltpu.roll(span, shift, 1)
                rows[group, which] = span[:, :padded].astype(jnp.bfloat16)

        return group

    def send_rows(group):
        @pl.when(outer)
        def _():
            row_copy(group).start()

    def cut(step, members):
        waiting = None
        for tasks in members:
            group = rows_of(step, tasks)
            if waiting is not None:
                send_rows(waiting)
            waiting = group
        return waiting

    def rows_arrive(step):
        @pl.when(inner)
        def _():
            for tasks in range(n_task):
                row_copy(product_order[step] * n_task + tasks).wait_recv()

    def multiply(step):
        rows_arrive(step)

        @pl.loop(0, 2)
        def _(which):
            piece = product(rows, held, product_order[step], which)
            if step == 0:
                total[which] = piece
            else:
                total[which] += piece

    sides = (task, task_x, task_y)
    everyone = sides + (task_d,)
    for which in range(2):
        own_step(0, which)
    for which in range(2):
        own_step(1, which)
        side_step(0, which)
    for which in range(2):
        own_step(2, which)
        side_step(1, which)
        diagonal_step(0, which)
    waiting = cut(0, everyone)
    for which in range(2):
        own_step(3, which)
        if which == 0:
            send_rows(waiting)
        side_step(2, which)
        diagonal_step(1, which)
    waiting = cut(1, everyone)
    for which in range(2):
        side_step(3, which)
        if which == 0:
            send_rows(waiting)
        diagonal_step(2, which)
    waiting = cut(2, everyone)
    multiply(0)
    send_rows(waiting)
    waiting = cut(3, sides)
    multiply(1)
    send_rows(waiting)
    for which in range(2):
        diagonal_step(3, which)
    waiting = cut(3, (task_d,))
    multiply(2)
    send_rows(waiting)
    rows_arrive(3)

    for out in started:
        out.wait_send()

    @pl.when(inner)
    def _():
        for which in range(2):
            to_inner(which).wait_send()
            relay(which).wait_send()

    @pl.when(outer)
    def _():
        for group in range(n_planes * n_task):
            row_copy(group).wait_send()


def gathered(hidden, attn_out, gain_attn, gain_mlp, lengths):
    _, tok_dev, width = hidden.shape
    n_tok, n_task = lax.axis_size("tok"), lax.axis_size("task")
    column_band = width // 2
    row_count = column_band // 2 // n_task
    padded = -(-row_count // LANES) * LANES
    devices = n_tok * n_task
    groups = devices // 2
    vmem, hbm = (pl.BlockSpec(memory_space=space) for space in (pltpu.VMEM, pltpu.HBM))
    semaphores = pltpu.SemaphoreType.DMA
    held, rows, total = pl.pallas_call(
        gather_kernel,
        out_shape=(
            jax.ShapeDtypeStruct((2, devices, tok_dev, column_band), jnp.bfloat16),
            jax.ShapeDtypeStruct((groups, 2, 2 * tok_dev, padded), jnp.bfloat16),
            jax.ShapeDtypeStruct((2, padded, column_band), jnp.float32),
        ),
        in_specs=[hbm] * 5,
        out_specs=(vmem,) * 3,
        scratch_shapes=[
            pltpu.VMEM(hidden.shape, jnp.bfloat16),
            pltpu.VMEM(attn_out.shape, jnp.bfloat16),
            pltpu.VMEM(gain_attn.shape, jnp.bfloat16),
            pltpu.VMEM(gain_mlp.shape, jnp.bfloat16),
            pltpu.SMEM(lengths.shape, jnp.int32),
            pltpu.VMEM((2, 2, tok_dev, column_band), jnp.bfloat16),
            semaphores((5,)),
            semaphores((2, devices)),
            semaphores((groups,)),
            semaphores((groups,)),
            semaphores((2, 4)),
            semaphores((2, 2, n_tok)),
            semaphores((2, devices)),
        ],
        compiler_params=pltpu.CompilerParams(
            collective_id=0, has_side_effects=True, vmem_limit_bytes=24 * 2**20
        ),
    )(*(
        pltpu.with_memory_space_constraint(array, pltpu.HBM)
        for array in (hidden, attn_out, gain_attn, gain_mlp, lengths)
    ))
    shape = (1, row_count, column_band)
    n_bands = 2
    return pl.pallas_call(
        last_kernel,
        out_shape=(jax.ShapeDtypeStruct(shape, jnp.float32),) * 2,
        in_specs=[vmem] * 3,
        out_specs=(hbm, hbm),
        scratch_shapes=[
            pltpu.VMEM((2,) + shape, jnp.float32),
            semaphores((2, n_bands)),
        ],
        compiler_params=pltpu.CompilerParams(vmem_limit_bytes=12 * 2**20),
    )(held, rows, total)


def from_partner(block, axis, distance):
    count = lax.axis_size(axis)
    route = []
    for low in range(count):
        high = low | 1 << distance
        if high != low and high < count:
            route += [(low, high), (high, low)]
    return lax.ppermute(block, axis, route)


def normed(values, gain):
    scale = lax.rsqrt(jnp.mean(values * values, axis=-1, keepdims=True) + 1e-06)
    return values * scale * gain.astype(jnp.float32)


def per_device(hidden, attn_out, gain_attn, gain_mlp, lengths):
    tok_dev = hidden.shape[1]
    width = hidden.shape[2]
    n_tok = lax.axis_size("tok")
    n_task = lax.axis_size("task")
    block_side = min(4, max(2, n_tok // 16))
    token_parts = n_tok // (block_side * block_side)
    if (n_task, n_tok, block_side) == (4, 8, 2) and width % (4 * LANES) == 0 and tok_dev % 16 == 0:
        return gathered(hidden, attn_out, gain_attn, gain_mlp, lengths)
    column_band = width // block_side
    tile_rows = column_band // token_parts
    slice_rows = tok_dev // token_parts
    seq_count = lengths.shape[1]
    seq_slots = tok_dev * n_tok // seq_count
    place = lax.axis_index("tok") * tok_dev + jnp.arange(tok_dev, dtype=jnp.int32)
    which = place // seq_slots
    offset = place % seq_slots
    owner = which[:, None] == jnp.arange(seq_count, dtype=jnp.int32)[None, :]
    limit = jnp.sum(jnp.where(owner, lengths[0][None, :], 0), axis=1)
    live = (offset < limit).astype(jnp.float32)[:, None]
    first = hidden[0].astype(jnp.float32)
    x_attn = (normed(first, gain_attn) * live).astype(jnp.bfloat16)
    mixed = first + attn_out[0].astype(jnp.float32)
    x_mlp = (normed(mixed, gain_mlp) * live).astype(jnp.bfloat16)

    def bands(values):
        split = values.reshape(token_parts, slice_rows, block_side, column_band).transpose(
            2, 0, 1, 3
        )
        shape = (block_side, block_side, token_parts, slice_rows, column_band)
        left_side = jnp.broadcast_to(split[:, None], shape).reshape(n_tok, slice_rows, column_band)
        right_side = jnp.broadcast_to(split[None], shape).reshape(n_tok, slice_rows, column_band)
        return (left_side, right_side)

    left_attn, right_attn = bands(x_attn)
    left_mlp, right_mlp = bands(x_mlp)
    arrived = (
        lax.all_to_all(left_attn, "tok", split_axis=0, concat_axis=0, tiled=True),
        lax.all_to_all(right_attn, "tok", split_axis=0, concat_axis=0, tiled=True),
        lax.all_to_all(left_mlp, "tok", split_axis=0, concat_axis=0, tiled=True),
        lax.all_to_all(right_mlp, "tok", split_axis=0, concat_axis=0, tiled=True),
    )
    contract = (((0, 1), (0, 1)), ((), ()))
    tile_attn = lax.dot_general(
        arrived[0], arrived[1], contract, preferred_element_type=jnp.float32
    )
    tile_mlp = lax.dot_general(arrived[2], arrived[3], contract, preferred_element_type=jnp.float32)
    grams = (
        tile_attn.reshape(token_parts, tile_rows, column_band),
        tile_mlp.reshape(token_parts, tile_rows, column_band),
    )
    part_index = lax.axis_index("tok") % token_parts
    depth_bits = token_parts.bit_length() - 1

    def halve(current, bit):
        upper_bit = part_index // (1 << bit) % 2 == 1
        middle = current[0].shape[0] // 2
        outgoing = tuple(
            (jnp.where(upper_bit, piece[:middle], piece[middle:]) for piece in current)
        )
        kept = tuple((jnp.where(upper_bit, piece[middle:], piece[:middle]) for piece in current))
        incoming = from_partner(outgoing, "tok", bit)
        return tuple((mine + theirs for mine, theirs in zip(kept, incoming)))

    for bit in range(depth_bits - 1, -1, -1):
        grams = halve(grams, bit)
    shaped = tuple((piece.reshape(n_task, tile_rows // n_task, column_band) for piece in grams))
    grams = lax.psum_scatter(shaped, "task", scatter_dimension=0, tiled=True)
    factor = 1.0 / (tok_dev * n_tok)
    final_attn = grams[0] * factor
    final_mlp = grams[1] * factor
    return (final_attn, final_mlp)


def solution(mesh):
    return jax.shard_map(
        per_device,
        mesh=mesh,
        in_specs=(P("task", "tok", None), P("task", "tok", None), P(), P(), P("task", None)),
        out_specs=(P("tok", "task", None), P("tok", "task", None)),
        check_vma=False,
    )
```

```python
import functools

import jax
import jax.numpy as jnp
from jax import lax
from jax.experimental import pallas as pl
from jax.experimental.pallas import tpu as pltpu
from jax.sharding import PartitionSpec as P

LANES = 128


def planes_in_product_order():
    plane = lax.axis_index("tok") // 2
    inner = jnp.logical_or(plane == 1, plane == 2)
    plane_1 = plane + 1 - 2 * (plane % 2)
    plane_2 = jnp.where(plane // 2 == 1, plane - 2, plane + 2)
    plane_3 = 3 - plane
    return (
        jnp.where(inner, plane_1, plane), jnp.where(inner, plane, plane_1),
        jnp.where(inner, plane_3, plane_2), jnp.where(inner, plane_2, plane_3),
    )


def product(rows, held, plane, which, columns=slice(None)):
    n_task = lax.axis_size("task")
    left = rows[pl.ds(plane * n_task, n_task), which]
    right = held[which, pl.ds(plane * 2 * n_task, 2 * n_task), :, columns]
    depth = left.shape[0] * left.shape[1]
    return lax.dot_general(
        left.reshape(depth, left.shape[2]), right.reshape(depth, right.shape[2]),
        (((0,), (0,)), ((), ())), preferred_element_type=jnp.float32,
    )


def last_kernel(held, rows, total, out_attn, out_mlp, staged, sent):
    row_count, column_band = out_attn.shape[1], out_attn.shape[2]
    plane = planes_in_product_order()[3]
    factor = 1.0 / (lax.axis_size("tok") * held.shape[2])
    n_bands = sent.shape[1]
    width = column_band // n_bands
    writes = []
    for which, out in ((0, out_attn), (1, out_mlp)):
        for band in range(n_bands):
            span = slice(band * width, (band + 1) * width)
            piece = total[which, :, span] + product(rows, held, plane, which, span)
            staged[which, 0, :, span] = piece[:row_count] * factor
            write = pltpu.make_async_copy(
                staged.at[which, :, :, span], out.at[:, :, span], sent.at[which, band]
            )
            write.start()
            writes.append(write)
    for write in writes:
        write.wait()


def gather_kernel(
    hidden_hbm, attn_hbm, gain_attn_hbm, gain_mlp_hbm, lengths_hbm, held, rows, total,
    hidden, attn_out, gain_attn, gain_mlp, lengths, mine, lent,
    loaded, got, row_got, row_sent, z_sent, side_sent, pair_sent,
):
    task, tok = lax.axis_index("task"), lax.axis_index("tok")
    n_task = lax.axis_size("task")
    plane, core = tok // 2, tok % 2
    band = plane % 2
    tok_dev, column_band = held.shape[2], held.shape[3]
    n_planes = held.shape[1] // (2 * n_task)
    inner = jnp.logical_or(plane == 1, plane == 2)
    outer = jnp.logical_not(inner)

    def flip(value, bit):
        return value + bit - 2 * bit * (value // bit % 2)

    task_x, task_y = flip(task, 1), flip(task, 2)
    task_d = flip(task_x, 2)
    plane_1, plane_2 = flip(plane, 1), flip(plane, 2)
    plane_3 = flip(plane_1, 2)
    near, far = jnp.where(inner, plane_3, plane_2), jnp.where(inner, plane_2, plane_3)
    order = (plane, plane_1, near, far)
    product_order = planes_in_product_order()

    def at(tasks, planes, cores):
        return {"task": tasks, "tok": planes * 2 + cores}

    def chunk(planes, tasks, cores):
        return planes * (2 * n_task) + tasks * 2 + cores

    own = chunk(plane, task, core)

    loads = [
        pltpu.make_async_copy(source, target, loaded.at[spot])
        for spot, (source, target) in enumerate((
            (hidden_hbm, hidden), (attn_hbm, attn_out), (gain_attn_hbm, gain_attn),
            (gain_mlp_hbm, gain_mlp), (lengths_hbm, lengths),
        ))
    ]
    for load in loads:
        load.start()
    peers = (
        at(task_x, plane, core), at(task_y, plane, core), at(task, plane, 1 - core),
        at(task, plane_1, core), at(task, plane_2, core), at(task, plane_3, core),
    )
    barrier = pltpu.get_barrier_semaphore()
    for peer in peers:
        pl.semaphore_signal(
            barrier, inc=1, device_id=peer, device_id_type=pl.DeviceIdType.MESH
        )
    for load in loads:
        load.wait()

    slab = 16
    seq_count = lengths.shape[1]
    seq_slots = tok_dev * lax.axis_size("tok") // seq_count
    for low in range(0, tok_dev, slab):
        part = pl.ds(low, slab)
        place = tok * tok_dev + low + lax.broadcasted_iota(jnp.int32, (slab, 1), 0)
        live = jnp.zeros((slab, 1), jnp.float32)
        for seq in range(seq_count):
            offset = place - seq * seq_slots
            inside = (offset >= 0) & (offset < seq_slots) & (offset < lengths[0, seq])
            live = jnp.where(inside, 1.0, live)
        first = hidden[0, part, :].astype(jnp.float32)
        mixed = first + attn_out[0, part, :].astype(jnp.float32)
        for which, values, gain in ((0, first, gain_attn), (1, mixed, gain_mlp)):
            done = (normed(values, gain[...].reshape(1, -1)) * live).astype(jnp.bfloat16)
            for side in range(2):
                mine[which, side, part, :] = done[:, side * column_band : (side + 1) * column_band]
    for which in range(2):
        held[which, own] = mine[which, band]

    pl.semaphore_wait(barrier, len(peers))
    to_x, to_y, to_pair, to_1, to_2, to_3 = peers

    def copy(source, which, q, sent, peer):
        return pltpu.make_async_remote_copy(
            src_ref=source, dst_ref=held.at[which, q], send_sem=sent,
            recv_sem=got.at[which, q], device_id=peer,
            device_id_type=pl.DeviceIdType.MESH,
        )

    started = []

    def send(*arguments):
        out = copy(*arguments)
        out.start()
        started.append(out)

    def arrive(which, q):
        copy(held.at[which, q], which, q, pair_sent.at[which, q], to_pair).wait_recv()

    def to_inner(which):
        return copy(mine.at[which, 1 - band], which, own, z_sent.at[which, 2], to_3)

    def relay(which):
        q = chunk(plane_1, task, core)
        return copy(held.at[which, q], which, q, z_sent.at[which, 3], to_2)

    def own_step(step, which):
        q = chunk(order[step], task, core)
        if step:
            arrive(which, q)
            source = held.at[which, q]
        else:
            source = mine.at[which, band]
        if step == 1:
            @pl.when(inner)
            def _():
                relay(which).start()
        send(source, which, q, side_sent.at[0, which, step], to_x)
        send(source, which, q, side_sent.at[1, which, step], to_y)
        if step == 0:
            @pl.when(inner)
            def _():
                to_inner(which).start()
            send(mine.at[which, 1 - band], which, own, z_sent.at[which, 0], to_1)
            send(source, which, own, z_sent.at[which, 1], to_2)
        send(source, which, q, pair_sent.at[which, q], to_pair)

    def side_step(step, which):
        for tasks, relayed, axis, peer in (
            (task_x, 0, 1, to_y), (task_y, 1, 0, to_x)
        ):
            q = chunk(order[step], tasks, core)
            arrive(which, q)
            if which == relayed:
                send(
                    held.at[which, q], which, q,
                    side_sent.at[axis, which, n_planes + step], peer,
                )
            send(held.at[which, q], which, q, pair_sent.at[which, q], to_pair)

    def diagonal_step(step, which):
        q = chunk(order[step], task_d, core)
        arrive(which, q)
        send(held.at[which, q], which, q, pair_sent.at[which, q], to_pair)

    row_count = column_band // 2 // n_task
    padded = rows.shape[3]
    window = min(padded + LANES, column_band)
    row_start = core * (column_band // 2) + task * row_count
    base = jnp.minimum(row_start // LANES * LANES, column_band - window)
    shift = window - (row_start - base)

    def row_copy(group):
        return pltpu.make_async_remote_copy(
            src_ref=rows.at[group], dst_ref=rows.at[group], send_sem=row_sent.at[group],
            recv_sem=row_got.at[group], device_id=to_1,
            device_id_type=pl.DeviceIdType.MESH,
        )

    def lend_copy(tasks):
        group = plane_1 * n_task + tasks
        return pltpu.make_async_remote_copy(
            src_ref=lent.at[tasks], dst_ref=rows.at[group], send_sem=row_sent.at[group],
            recv_sem=row_got.at[group], device_id=to_3,
            device_id_type=pl.DeviceIdType.MESH,
        )

    def rows_of(step, tasks):
        for which in range(2):
            arrive(which, chunk(order[step], tasks, 1 - core))
        group = order[step] * n_task + tasks

        def cut_into(target):
            for which in range(2):
                span = held[
                    which, pl.ds(group * 2, 2), :, pl.ds(pl.multiple_of(base, LANES), window)
                ]
                span = span.reshape(2 * tok_dev, window).astype(jnp.float32)
                span = pltpu.roll(span, shift, 1)
                target[which] = span[:, :padded].astype(jnp.bfloat16)

        @pl.when(outer)
        def _():
            cut_into(rows.at[group])

        if step == 1:
            @pl.when(inner)
            def _():
                cut_into(lent.at[tasks])

        return step, tasks, group

    def send_rows(waiting):
        step, tasks, group = waiting
        if step < n_planes - 1:
            @pl.when(outer)
            def _():
                row_copy(group).start()

        if step == 1:
            @pl.when(inner)
            def _():
                lend_copy(tasks).start()

    def cut(step, members):
        waiting = None
        for tasks in members:
            group = rows_of(step, tasks)
            if waiting is not None:
                send_rows(waiting)
            waiting = group
        return waiting

    def rows_arrive(step):
        @pl.when(inner)
        def _():
            for tasks in range(n_task):
                row_copy(product_order[step] * n_task + tasks).wait_recv()

    def multiply(step):
        rows_arrive(step)

        @pl.loop(0, 2)
        def _(which):
            piece = product(rows, held, product_order[step], which)
            if step == 0:
                total[which] = piece
            else:
                total[which] += piece

    sides = (task, task_x, task_y)
    everyone = sides + (task_d,)
    for which in range(2):
        own_step(0, which)
    for which in range(2):
        own_step(1, which)
        side_step(0, which)
    for which in range(2):
        own_step(2, which)
        side_step(1, which)
        diagonal_step(0, which)
    waiting = cut(0, everyone)
    for which in range(2):
        own_step(3, which)
        if which == 0:
            send_rows(waiting)
        side_step(2, which)
        diagonal_step(1, which)
    waiting = cut(1, everyone)
    for which in range(2):
        side_step(3, which)
        if which == 0:
            send_rows(waiting)
        diagonal_step(2, which)
    waiting = cut(2, everyone)
    multiply(0)
    send_rows(waiting)
    waiting = cut(3, sides)
    multiply(1)
    send_rows(waiting)
    for which in range(2):
        diagonal_step(3, which)
    waiting = cut(3, (task_d,))
    multiply(2)
    send_rows(waiting)
    rows_arrive(3)

    for out in started:
        out.wait_send()

    @pl.when(inner)
    def _():
        for which in range(2):
            to_inner(which).wait_send()
            relay(which).wait_send()
        for tasks in range(n_task):
            lend_copy(tasks).wait_send()

    @pl.when(outer)
    def _():
        for step in range(n_planes - 1):
            for tasks in range(n_task):
                row_copy(order[step] * n_task + tasks).wait_send()


def gathered(hidden, attn_out, gain_attn, gain_mlp, lengths):
    _, tok_dev, width = hidden.shape
    n_tok, n_task = lax.axis_size("tok"), lax.axis_size("task")
    column_band = width // 2
    row_count = column_band // 2 // n_task
    padded = -(-row_count // LANES) * LANES
    devices = n_tok * n_task
    groups = devices // 2
    vmem, hbm = (pl.BlockSpec(memory_space=space) for space in (pltpu.VMEM, pltpu.HBM))
    semaphores = pltpu.SemaphoreType.DMA
    held, rows, total = pl.pallas_call(
        gather_kernel,
        out_shape=(
            jax.ShapeDtypeStruct((2, devices, tok_dev, column_band), jnp.bfloat16),
            jax.ShapeDtypeStruct((groups, 2, 2 * tok_dev, padded), jnp.bfloat16),
            jax.ShapeDtypeStruct((2, padded, column_band), jnp.float32),
        ),
        in_specs=[hbm] * 5,
        out_specs=(vmem,) * 3,
        scratch_shapes=[
            pltpu.VMEM(hidden.shape, jnp.bfloat16),
            pltpu.VMEM(attn_out.shape, jnp.bfloat16),
            pltpu.VMEM(gain_attn.shape, jnp.bfloat16),
            pltpu.VMEM(gain_mlp.shape, jnp.bfloat16),
            pltpu.SMEM(lengths.shape, jnp.int32),
            pltpu.VMEM((2, 2, tok_dev, column_band), jnp.bfloat16),
            pltpu.VMEM((n_task, 2, 2 * tok_dev, padded), jnp.bfloat16),
            semaphores((5,)),
            semaphores((2, devices)),
            semaphores((groups,)),
            semaphores((groups,)),
            semaphores((2, 4)),
            semaphores((2, 2, n_tok)),
            semaphores((2, devices)),
        ],
        compiler_params=pltpu.CompilerParams(
            collective_id=0, has_side_effects=True, vmem_limit_bytes=24 * 2**20
        ),
    )(*(
        pltpu.with_memory_space_constraint(array, pltpu.HBM)
        for array in (hidden, attn_out, gain_attn, gain_mlp, lengths)
    ))
    shape = (1, row_count, column_band)
    n_bands = 2
    return pl.pallas_call(
        last_kernel,
        out_shape=(jax.ShapeDtypeStruct(shape, jnp.float32),) * 2,
        in_specs=[vmem] * 3,
        out_specs=(hbm, hbm),
        scratch_shapes=[
            pltpu.VMEM((2,) + shape, jnp.float32),
            semaphores((2, n_bands)),
        ],
        compiler_params=pltpu.CompilerParams(vmem_limit_bytes=12 * 2**20),
    )(held, rows, total)


def from_partner(block, axis, distance):
    count = lax.axis_size(axis)
    route = []
    for low in range(count):
        high = low | 1 << distance
        if high != low and high < count:
            route += [(low, high), (high, low)]
    return lax.ppermute(block, axis, route)


def normed(values, gain):
    scale = lax.rsqrt(jnp.mean(values * values, axis=-1, keepdims=True) + 1e-06)
    return values * scale * gain.astype(jnp.float32)


def per_device(hidden, attn_out, gain_attn, gain_mlp, lengths):
    tok_dev = hidden.shape[1]
    width = hidden.shape[2]
    n_tok = lax.axis_size("tok")
    n_task = lax.axis_size("task")
    block_side = min(4, max(2, n_tok // 16))
    token_parts = n_tok // (block_side * block_side)
    if (n_task, n_tok, block_side) == (4, 8, 2) and width % (4 * LANES) == 0 and tok_dev % 16 == 0:
        return gathered(hidden, attn_out, gain_attn, gain_mlp, lengths)
    column_band = width // block_side
    tile_rows = column_band // token_parts
    slice_rows = tok_dev // token_parts
    seq_count = lengths.shape[1]
    seq_slots = tok_dev * n_tok // seq_count
    place = lax.axis_index("tok") * tok_dev + jnp.arange(tok_dev, dtype=jnp.int32)
    which = place // seq_slots
    offset = place % seq_slots
    owner = which[:, None] == jnp.arange(seq_count, dtype=jnp.int32)[None, :]
    limit = jnp.sum(jnp.where(owner, lengths[0][None, :], 0), axis=1)
    live = (offset < limit).astype(jnp.float32)[:, None]
    first = hidden[0].astype(jnp.float32)
    x_attn = (normed(first, gain_attn) * live).astype(jnp.bfloat16)
    mixed = first + attn_out[0].astype(jnp.float32)
    x_mlp = (normed(mixed, gain_mlp) * live).astype(jnp.bfloat16)

    def bands(values):
        split = values.reshape(token_parts, slice_rows, block_side, column_band).transpose(
            2, 0, 1, 3
        )
        shape = (block_side, block_side, token_parts, slice_rows, column_band)
        left_side = jnp.broadcast_to(split[:, None], shape).reshape(n_tok, slice_rows, column_band)
        right_side = jnp.broadcast_to(split[None], shape).reshape(n_tok, slice_rows, column_band)
        return (left_side, right_side)

    left_attn, right_attn = bands(x_attn)
    left_mlp, right_mlp = bands(x_mlp)
    arrived = (
        lax.all_to_all(left_attn, "tok", split_axis=0, concat_axis=0, tiled=True),
        lax.all_to_all(right_attn, "tok", split_axis=0, concat_axis=0, tiled=True),
        lax.all_to_all(left_mlp, "tok", split_axis=0, concat_axis=0, tiled=True),
        lax.all_to_all(right_mlp, "tok", split_axis=0, concat_axis=0, tiled=True),
    )
    contract = (((0, 1), (0, 1)), ((), ()))
    tile_attn = lax.dot_general(
        arrived[0], arrived[1], contract, preferred_element_type=jnp.float32
    )
    tile_mlp = lax.dot_general(arrived[2], arrived[3], contract, preferred_element_type=jnp.float32)
    grams = (
        tile_attn.reshape(token_parts, tile_rows, column_band),
        tile_mlp.reshape(token_parts, tile_rows, column_band),
    )
    part_index = lax.axis_index("tok") % token_parts
    depth_bits = token_parts.bit_length() - 1

    def halve(current, bit):
        upper_bit = part_index // (1 << bit) % 2 == 1
        middle = current[0].shape[0] // 2
        outgoing = tuple(
            (jnp.where(upper_bit, piece[:middle], piece[middle:]) for piece in current)
        )
        kept = tuple((jnp.where(upper_bit, piece[middle:], piece[:middle]) for piece in current))
        incoming = from_partner(outgoing, "tok", bit)
        return tuple((mine + theirs for mine, theirs in zip(kept, incoming)))

    for bit in range(depth_bits - 1, -1, -1):
        grams = halve(grams, bit)
    shaped = tuple((piece.reshape(n_task, tile_rows // n_task, column_band) for piece in grams))
    grams = lax.psum_scatter(shaped, "task", scatter_dimension=0, tiled=True)
    factor = 1.0 / (tok_dev * n_tok)
    final_attn = grams[0] * factor
    final_mlp = grams[1] * factor
    return (final_attn, final_mlp)


def solution(mesh):
    return jax.shard_map(
        per_device,
        mesh=mesh,
        in_specs=(P("task", "tok", None), P("task", "tok", None), P(), P(), P("task", None)),
        out_specs=(P("tok", "task", None), P("tok", "task", None)),
        check_vma=False,
    )
```

```python
import functools

import jax
import jax.numpy as jnp
from jax import lax
from jax.experimental import pallas as pl
from jax.experimental.pallas import tpu as pltpu
from jax.sharding import PartitionSpec as P

LANES = 128
LENT = (2, 3)


def planes_in_product_order():
    plane = lax.axis_index("tok") // 2
    inner = jnp.logical_or(plane == 1, plane == 2)
    plane_1 = plane + 1 - 2 * (plane % 2)
    plane_2 = jnp.where(plane // 2 == 1, plane - 2, plane + 2)
    plane_3 = 3 - plane
    return (
        jnp.where(inner, plane_1, plane), jnp.where(inner, plane, plane_1),
        jnp.where(inner, plane_3, plane_2), jnp.where(inner, plane_2, plane_3),
    )


def product(rows, held, plane, which, columns=slice(None)):
    n_task = lax.axis_size("task")
    left = rows[pl.ds(plane * n_task, n_task), which]
    right = held[which, pl.ds(plane * 2 * n_task, 2 * n_task), :, columns]
    depth = left.shape[0] * left.shape[1]
    return lax.dot_general(
        left.reshape(depth, left.shape[2]), right.reshape(depth, right.shape[2]),
        (((0,), (0,)), ((), ())), preferred_element_type=jnp.float32,
    )


def last_kernel(held, rows, total, out_attn, out_mlp, staged, sent):
    row_count, column_band = out_attn.shape[1], out_attn.shape[2]
    plane = planes_in_product_order()[3]
    factor = 1.0 / (lax.axis_size("tok") * held.shape[2])
    n_bands = sent.shape[1]
    width = column_band // n_bands
    writes = []
    for which, out in ((0, out_attn), (1, out_mlp)):
        for band in range(n_bands):
            span = slice(band * width, (band + 1) * width)
            piece = total[which, :, span] + product(rows, held, plane, which, span)
            staged[which, 0, :, span] = piece[:row_count] * factor
            write = pltpu.make_async_copy(
                staged.at[which, :, :, span], out.at[:, :, span], sent.at[which, band]
            )
            write.start()
            writes.append(write)
    for write in writes:
        write.wait()


def gather_kernel(
    hidden_hbm, attn_hbm, gain_attn_hbm, gain_mlp_hbm, lengths_hbm, held, rows, total,
    hidden, attn_out, gain_attn, gain_mlp, lengths, mine, lent,
    loaded, got, row_got, row_sent, z_sent, side_sent, pair_sent,
):
    task, tok = lax.axis_index("task"), lax.axis_index("tok")
    n_task = lax.axis_size("task")
    plane, core = tok // 2, tok % 2
    band = plane % 2
    tok_dev, column_band = held.shape[2], held.shape[3]
    n_planes = held.shape[1] // (2 * n_task)
    inner = jnp.logical_or(plane == 1, plane == 2)
    outer = jnp.logical_not(inner)

    def flip(value, bit):
        return value + bit - 2 * bit * (value // bit % 2)

    task_x, task_y = flip(task, 1), flip(task, 2)
    task_d = flip(task_x, 2)
    plane_1, plane_2 = flip(plane, 1), flip(plane, 2)
    plane_3 = flip(plane_1, 2)
    near, far = jnp.where(inner, plane_3, plane_2), jnp.where(inner, plane_2, plane_3)
    order = (plane, plane_1, near, far)
    product_order = planes_in_product_order()

    def at(tasks, planes, cores):
        return {"task": tasks, "tok": planes * 2 + cores}

    def chunk(planes, tasks, cores):
        return planes * (2 * n_task) + tasks * 2 + cores

    own = chunk(plane, task, core)

    loads = [
        pltpu.make_async_copy(source, target, loaded.at[spot])
        for spot, (source, target) in enumerate((
            (hidden_hbm, hidden), (attn_hbm, attn_out), (gain_attn_hbm, gain_attn),
            (gain_mlp_hbm, gain_mlp), (lengths_hbm, lengths),
        ))
    ]
    for load in loads:
        load.start()
    peers = (
        at(task_x, plane, core), at(task_y, plane, core), at(task, plane, 1 - core),
        at(task, plane_1, core), at(task, plane_2, core), at(task, plane_3, core),
    )
    barrier = pltpu.get_barrier_semaphore()
    for peer in peers:
        pl.semaphore_signal(
            barrier, inc=1, device_id=peer, device_id_type=pl.DeviceIdType.MESH
        )
    for load in loads:
        load.wait()

    slab = 16
    seq_count = lengths.shape[1]
    seq_slots = tok_dev * lax.axis_size("tok") // seq_count
    for low in range(0, tok_dev, slab):
        part = pl.ds(low, slab)
        place = tok * tok_dev + low + lax.broadcasted_iota(jnp.int32, (slab, 1), 0)
        live = jnp.zeros((slab, 1), jnp.float32)
        for seq in range(seq_count):
            offset = place - seq * seq_slots
            inside = (offset >= 0) & (offset < seq_slots) & (offset < lengths[0, seq])
            live = jnp.where(inside, 1.0, live)
        first = hidden[0, part, :].astype(jnp.float32)
        mixed = first + attn_out[0, part, :].astype(jnp.float32)
        for which, values, gain in ((0, first, gain_attn), (1, mixed, gain_mlp)):
            done = (normed(values, gain[...].reshape(1, -1)) * live).astype(jnp.bfloat16)
            for side in range(2):
                mine[which, side, part, :] = done[:, side * column_band : (side + 1) * column_band]
    for which in range(2):
        held[which, own] = mine[which, band]

    pl.semaphore_wait(barrier, len(peers))
    to_x, to_y, to_pair, to_1, to_2, to_3 = peers

    def copy(source, which, q, sent, peer):
        return pltpu.make_async_remote_copy(
            src_ref=source, dst_ref=held.at[which, q], send_sem=sent,
            recv_sem=got.at[which, q], device_id=peer,
            device_id_type=pl.DeviceIdType.MESH,
        )

    started = []

    def send(*arguments):
        out = copy(*arguments)
        out.start()
        started.append(out)

    def arrive(which, q):
        copy(held.at[which, q], which, q, pair_sent.at[which, q], to_pair).wait_recv()

    def to_inner(which):
        return copy(mine.at[which, 1 - band], which, own, z_sent.at[which, 2], to_3)

    def relay(which):
        q = chunk(plane_1, task, core)
        return copy(held.at[which, q], which, q, z_sent.at[which, 3], to_2)

    def own_step(step, which):
        q = chunk(order[step], task, core)
        if step:
            arrive(which, q)
            source = held.at[which, q]
        else:
            source = mine.at[which, band]
        if step == 1:
            @pl.when(inner)
            def _():
                relay(which).start()
        send(source, which, q, side_sent.at[0, which, step], to_x)
        send(source, which, q, side_sent.at[1, which, step], to_y)
        if step == 0:
            @pl.when(inner)
            def _():
                to_inner(which).start()
            send(mine.at[which, 1 - band], which, own, z_sent.at[which, 0], to_1)
            send(source, which, own, z_sent.at[which, 1], to_2)
        send(source, which, q, pair_sent.at[which, q], to_pair)

    def side_step(step, which):
        for tasks, relayed, axis, peer in (
            (task_x, 0, 1, to_y), (task_y, 1, 0, to_x)
        ):
            q = chunk(order[step], tasks, core)
            arrive(which, q)
            if which == relayed:
                send(
                    held.at[which, q], which, q,
                    side_sent.at[axis, which, n_planes + step], peer,
                )
            send(held.at[which, q], which, q, pair_sent.at[which, q], to_pair)

    def diagonal_step(step, which):
        q = chunk(order[step], task_d, core)
        arrive(which, q)
        send(held.at[which, q], which, q, pair_sent.at[which, q], to_pair)

    row_count = column_band // 2 // n_task
    padded = rows.shape[3]
    window = min(padded + LANES, column_band)
    row_start = core * (column_band // 2) + task * row_count
    base = jnp.minimum(row_start // LANES * LANES, column_band - window)
    shift = window - (row_start - base)

    def row_copy(group):
        return pltpu.make_async_remote_copy(
            src_ref=rows.at[group], dst_ref=rows.at[group], send_sem=row_sent.at[group],
            recv_sem=row_got.at[group], device_id=to_1,
            device_id_type=pl.DeviceIdType.MESH,
        )

    everyone = (task, task_x, task_y, task_d)
    lends = [(1, member) for member in range(4)] + [(0, member) for member in LENT]
    gives = [
        (step, member) for step in range(n_planes - 1) for member in range(4)
        if step < 2 or (0, member) not in lends
    ]

    def lend_copy(step, tasks):
        group = order[step] * n_task + tasks
        return pltpu.make_async_remote_copy(
            src_ref=lent.at[step, tasks], dst_ref=rows.at[group], send_sem=row_sent.at[group],
            recv_sem=row_got.at[group], device_id=to_3,
            device_id_type=pl.DeviceIdType.MESH,
        )

    def rows_of(step, member):
        tasks = everyone[member]
        for which in range(2):
            arrive(which, chunk(order[step], tasks, 1 - core))
        group = order[step] * n_task + tasks

        def cut_into(target):
            for which in range(2):
                span = held[
                    which, pl.ds(group * 2, 2), :, pl.ds(pl.multiple_of(base, LANES), window)
                ]
                span = span.reshape(2 * tok_dev, window).astype(jnp.float32)
                span = pltpu.roll(span, shift, 1)
                target[which] = span[:, :padded].astype(jnp.bfloat16)

        @pl.when(outer)
        def _():
            cut_into(rows.at[group])

        if (step, member) in lends:
            @pl.when(inner)
            def _():
                cut_into(lent.at[step, tasks])

        return step, member, group

    def send_rows(waiting):
        step, member, group = waiting
        if (step, member) in gives:
            @pl.when(outer)
            def _():
                row_copy(group).start()

        if (step, member) in lends:
            @pl.when(inner)
            def _():
                lend_copy(step, everyone[member]).start()

    def cut(step, members):
        waiting = None
        for member in members:
            group = rows_of(step, member)
            if waiting is not None:
                send_rows(waiting)
            waiting = group
        return waiting

    def rows_arrive(step):
        @pl.when(inner)
        def _():
            for tasks in range(n_task):
                row_copy(product_order[step] * n_task + tasks).wait_recv()

    def multiply(step):
        rows_arrive(step)

        @pl.loop(0, 2)
        def _(which):
            piece = product(rows, held, product_order[step], which)
            if step == 0:
                total[which] = piece
            else:
                total[which] += piece

    every, sides = range(4), range(3)
    for which in range(2):
        own_step(0, which)
    for which in range(2):
        side_step(0, which)
        own_step(1, which)
    for which in range(2):
        side_step(1, which)
        own_step(2, which)
        diagonal_step(0, which)
    waiting = cut(0, every)
    for which in range(2):
        side_step(2, which)
        if which == 0:
            send_rows(waiting)
        own_step(3, which)
        diagonal_step(1, which)
    waiting = cut(1, every)
    for which in range(2):
        side_step(3, which)
        if which == 0:
            send_rows(waiting)
        diagonal_step(2, which)
    waiting = cut(2, every)
    multiply(0)
    send_rows(waiting)
    waiting = cut(3, sides)
    multiply(1)
    send_rows(waiting)
    for which in range(2):
        diagonal_step(3, which)
    multiply(2)
    cut(3, (3,))
    rows_arrive(3)

    for out in started:
        out.wait_send()

    @pl.when(inner)
    def _():
        for which in range(2):
            to_inner(which).wait_send()
            relay(which).wait_send()
        for step, member in lends:
            lend_copy(step, everyone[member]).wait_send()

    @pl.when(outer)
    def _():
        for step, member in gives:
            row_copy(order[step] * n_task + everyone[member]).wait_send()


def gathered(hidden, attn_out, gain_attn, gain_mlp, lengths):
    _, tok_dev, width = hidden.shape
    n_tok, n_task = lax.axis_size("tok"), lax.axis_size("task")
    column_band = width // 2
    row_count = column_band // 2 // n_task
    padded = -(-row_count // LANES) * LANES
    devices = n_tok * n_task
    groups = devices // 2
    vmem, hbm = (pl.BlockSpec(memory_space=space) for space in (pltpu.VMEM, pltpu.HBM))
    semaphores = pltpu.SemaphoreType.DMA
    held, rows, total = pl.pallas_call(
        gather_kernel,
        out_shape=(
            jax.ShapeDtypeStruct((2, devices, tok_dev, column_band), jnp.bfloat16),
            jax.ShapeDtypeStruct((groups, 2, 2 * tok_dev, padded), jnp.bfloat16),
            jax.ShapeDtypeStruct((2, padded, column_band), jnp.float32),
        ),
        in_specs=[hbm] * 5,
        out_specs=(vmem,) * 3,
        scratch_shapes=[
            pltpu.VMEM(hidden.shape, jnp.bfloat16),
            pltpu.VMEM(attn_out.shape, jnp.bfloat16),
            pltpu.VMEM(gain_attn.shape, jnp.bfloat16),
            pltpu.VMEM(gain_mlp.shape, jnp.bfloat16),
            pltpu.SMEM(lengths.shape, jnp.int32),
            pltpu.VMEM((2, 2, tok_dev, column_band), jnp.bfloat16),
            pltpu.VMEM((2, n_task, 2, 2 * tok_dev, padded), jnp.bfloat16),
            semaphores((5,)),
            semaphores((2, devices)),
            semaphores((groups,)),
            semaphores((groups,)),
            semaphores((2, 4)),
            semaphores((2, 2, n_tok)),
            semaphores((2, devices)),
        ],
        compiler_params=pltpu.CompilerParams(
            collective_id=0, has_side_effects=True, vmem_limit_bytes=24 * 2**20
        ),
    )(*(
        pltpu.with_memory_space_constraint(array, pltpu.HBM)
        for array in (hidden, attn_out, gain_attn, gain_mlp, lengths)
    ))
    shape = (1, row_count, column_band)
    n_bands = 2
    return pl.pallas_call(
        last_kernel,
        out_shape=(jax.ShapeDtypeStruct(shape, jnp.float32),) * 2,
        in_specs=[vmem] * 3,
        out_specs=(hbm, hbm),
        scratch_shapes=[
            pltpu.VMEM((2,) + shape, jnp.float32),
            semaphores((2, n_bands)),
        ],
        compiler_params=pltpu.CompilerParams(vmem_limit_bytes=12 * 2**20),
    )(held, rows, total)


def from_partner(block, axis, distance):
    count = lax.axis_size(axis)
    route = []
    for low in range(count):
        high = low | 1 << distance
        if high != low and high < count:
            route += [(low, high), (high, low)]
    return lax.ppermute(block, axis, route)


def normed(values, gain):
    scale = lax.rsqrt(jnp.mean(values * values, axis=-1, keepdims=True) + 1e-06)
    return values * scale * gain.astype(jnp.float32)


def per_device(hidden, attn_out, gain_attn, gain_mlp, lengths):
    tok_dev = hidden.shape[1]
    width = hidden.shape[2]
    n_tok = lax.axis_size("tok")
    n_task = lax.axis_size("task")
    block_side = min(4, max(2, n_tok // 16))
    token_parts = n_tok // (block_side * block_side)
    if (n_task, n_tok, block_side) == (4, 8, 2) and width % (4 * LANES) == 0 and tok_dev % 16 == 0:
        return gathered(hidden, attn_out, gain_attn, gain_mlp, lengths)
    column_band = width // block_side
    tile_rows = column_band // token_parts
    slice_rows = tok_dev // token_parts
    seq_count = lengths.shape[1]
    seq_slots = tok_dev * n_tok // seq_count
    place = lax.axis_index("tok") * tok_dev + jnp.arange(tok_dev, dtype=jnp.int32)
    which = place // seq_slots
    offset = place % seq_slots
    owner = which[:, None] == jnp.arange(seq_count, dtype=jnp.int32)[None, :]
    limit = jnp.sum(jnp.where(owner, lengths[0][None, :], 0), axis=1)
    live = (offset < limit).astype(jnp.float32)[:, None]
    first = hidden[0].astype(jnp.float32)
    x_attn = (normed(first, gain_attn) * live).astype(jnp.bfloat16)
    mixed = first + attn_out[0].astype(jnp.float32)
    x_mlp = (normed(mixed, gain_mlp) * live).astype(jnp.bfloat16)

    def bands(values):
        split = values.reshape(token_parts, slice_rows, block_side, column_band).transpose(
            2, 0, 1, 3
        )
        shape = (block_side, block_side, token_parts, slice_rows, column_band)
        left_side = jnp.broadcast_to(split[:, None], shape).reshape(n_tok, slice_rows, column_band)
        right_side = jnp.broadcast_to(split[None], shape).reshape(n_tok, slice_rows, column_band)
        return (left_side, right_side)

    left_attn, right_attn = bands(x_attn)
    left_mlp, right_mlp = bands(x_mlp)
    arrived = (
        lax.all_to_all(left_attn, "tok", split_axis=0, concat_axis=0, tiled=True),
        lax.all_to_all(right_attn, "tok", split_axis=0, concat_axis=0, tiled=True),
        lax.all_to_all(left_mlp, "tok", split_axis=0, concat_axis=0, tiled=True),
        lax.all_to_all(right_mlp, "tok", split_axis=0, concat_axis=0, tiled=True),
    )
    contract = (((0, 1), (0, 1)), ((), ()))
    tile_attn = lax.dot_general(
        arrived[0], arrived[1], contract, preferred_element_type=jnp.float32
    )
    tile_mlp = lax.dot_general(arrived[2], arrived[3], contract, preferred_element_type=jnp.float32)
    grams = (
        tile_attn.reshape(token_parts, tile_rows, column_band),
        tile_mlp.reshape(token_parts, tile_rows, column_band),
    )
    part_index = lax.axis_index("tok") % token_parts
    depth_bits = token_parts.bit_length() - 1

    def halve(current, bit):
        upper_bit = part_index // (1 << bit) % 2 == 1
        middle = current[0].shape[0] // 2
        outgoing = tuple(
            (jnp.where(upper_bit, piece[:middle], piece[middle:]) for piece in current)
        )
        kept = tuple((jnp.where(upper_bit, piece[middle:], piece[:middle]) for piece in current))
        incoming = from_partner(outgoing, "tok", bit)
        return tuple((mine + theirs for mine, theirs in zip(kept, incoming)))

    for bit in range(depth_bits - 1, -1, -1):
        grams = halve(grams, bit)
    shaped = tuple((piece.reshape(n_task, tile_rows // n_task, column_band) for piece in grams))
    grams = lax.psum_scatter(shaped, "task", scatter_dimension=0, tiled=True)
    factor = 1.0 / (tok_dev * n_tok)
    final_attn = grams[0] * factor
    final_mlp = grams[1] * factor
    return (final_attn, final_mlp)


def solution(mesh):
    return jax.shard_map(
        per_device,
        mesh=mesh,
        in_specs=(P("task", "tok", None), P("task", "tok", None), P(), P(), P("task", None)),
        out_specs=(P("tok", "task", None), P("tok", "task", None)),
        check_vma=False,
    )
```
